8 devices in a mesh: dp: 2 (over z, y), ep: 4 (over x, core).
Axes of the slice: x: 2, y: 2, z: 1, core: 2. Of those that a mesh axis runs over, the one named last changes fastest.
Arguments:
- hidden: bfloat16 [32768, 2304], P(('dp', 'ep')), parts along dimension 0
- ln_gamma: float32 [2304], replicated
- ln_beta: float32 [2304], replicated
- w_router: bfloat16 [2304, 8], replicated
- w_gate: bfloat16 [8, 2304, 5760], P('ep')
- w_up: bfloat16 [8, 2304, 5760], P('ep')
- w_down: bfloat16 [8, 5760, 2304], P('ep')
- choice: int32 [32768, 2], P(('dp', 'ep')), parts along dimension 0
- mask_first: int32 [32768, 8], P(('dp', 'ep')), parts along dimension 0
- mask_second: int32 [32768, 8], P(('dp', 'ep')), parts along dimension 0
Outputs:
- output: bfloat16 [32768, 2304], P(('dp', 'ep')), parts along dimension 0
There are 2 independent parts. The reference program is written for one: setup_inputs(seed, part) draws one part's arguments, and reference() takes and returns one part's arrays. A program takes and returns all parts, laid end to end along the dimension named above; an argument that names none is the same for every part.
All inputs are finite; a program needn't handle non-finite values.
Results may differ from the reference program's by a relative error of at most 0.001.
Values are sent between devices in bfloat16 or wider.
A program may use at most 1 GiB of HBM per device.

```python
import jax
import jax.numpy as jnp
from jax import lax

D_MODEL = 2304
FF_WIDTH = 5760
EXPERTS = 8
TOKENS_DEV = 4096
GROUP_DEVS = 4
TOKENS = GROUP_DEVS * TOKENS_DEV
CAPACITY = (10 * TOKENS_DEV + 4 * EXPERTS - 1) // (4 * EXPERTS)
LN_EPS = 1e-5


def draw_routing(route_key):
    sub_keys = jax.random.split(route_key, 6)
    favoured = jax.random.randint(sub_keys[0], (), 0, EXPERTS)
    coin_flip = jax.random.randint(sub_keys[1], (TOKENS,), 0, 4)
    spread = jax.random.randint(sub_keys[2], (TOKENS,), 0, EXPERTS)
    first_pick = jnp.where(coin_flip == 0, favoured, spread)
    second_pick = (first_pick + 1 + jax.random.randint(sub_keys[3], (TOKENS,), 0, EXPERTS - 1)) % EXPERTS
    expert_ids = jnp.arange(EXPERTS)
    is_first = first_pick[:, None] == expert_ids
    is_second = second_pick[:, None] == expert_ids
    keep_first = jax.random.randint(sub_keys[4], (TOKENS, EXPERTS), 0, 4) == 0
    keep_second = jax.random.randint(sub_keys[5], (TOKENS, EXPERTS), 0, 4) == 0
    mask_first = (keep_first | is_first).astype(jnp.int32)
    mask_second = ((keep_second | is_second) & (~is_first)).astype(jnp.int32)
    choice = jnp.stack([first_pick, second_pick], axis=1).astype(jnp.int32)
    return choice, mask_first, mask_second


def setup_inputs(seed: int = 0, part: int = 0) -> dict:
    shared_keys = jax.random.split(jax.random.key(seed), 6)
    part_keys = jax.random.split(jax.random.fold_in(jax.random.key(seed + 1), part), 2)
    hidden = jax.random.normal(part_keys[0], (TOKENS, D_MODEL), jnp.float32).astype(jnp.bfloat16)
    choice, mask_first, mask_second = draw_routing(part_keys[1])
    ln_gamma = 1.0 + 0.4 * jax.random.normal(shared_keys[0], (D_MODEL,), jnp.float32)
    ln_beta = 0.4 * jax.random.normal(shared_keys[1], (D_MODEL,), jnp.float32)
    w_router = (jax.random.normal(shared_keys[2], (D_MODEL, EXPERTS), jnp.float32) * D_MODEL ** -0.5).astype(jnp.bfloat16)
    w_gate = (jax.random.normal(shared_keys[3], (EXPERTS, D_MODEL, FF_WIDTH), jnp.float32) * D_MODEL ** -0.5).astype(jnp.bfloat16)
    w_up = (jax.random.normal(shared_keys[4], (EXPERTS, D_MODEL, FF_WIDTH), jnp.float32) * D_MODEL ** -0.5).astype(jnp.bfloat16)
    w_down = (jax.random.normal(shared_keys[5], (EXPERTS, FF_WIDTH, D_MODEL), jnp.float32) * FF_WIDTH ** -0.5).astype(jnp.bfloat16)
    return {"hidden": hidden, "ln_gamma": ln_gamma, "ln_beta": ln_beta, "w_router": w_router,
            "w_gate": w_gate, "w_up": w_up, "w_down": w_down, "choice": choice,
            "mask_first": mask_first, "mask_second": mask_second}


def layer_norm(token_rows, ln_gamma, ln_beta):
    values = token_rows.astype(jnp.float32)
    centred = values - jnp.mean(values, axis=-1, keepdims=True)
    variance = jnp.mean(centred * centred, axis=-1, keepdims=True)
    return (centred * lax.rsqrt(variance + LN_EPS) * ln_gamma + ln_beta).astype(jnp.bfloat16)


def reference(hidden, ln_gamma, ln_beta, w_router, w_gate, w_up, w_down, choice, mask_first, mask_second):
    normed = layer_norm(hidden, ln_gamma, ln_beta)
    scores = jnp.dot(normed, w_router, preferred_element_type=jnp.float32)
    mask_pair = jnp.stack([mask_first, mask_second], axis=1) > 0
    soft_probs = jax.nn.softmax(jnp.where(mask_pair, scores[:, None, :], -jnp.inf), axis=-1)
    gate_vals = jnp.take_along_axis(soft_probs, choice[:, :, None], axis=-1)[:, :, 0]
    by_source = choice.reshape(GROUP_DEVS, TOKENS_DEV, 2)
    expert_ids = jnp.arange(EXPERTS, dtype=jnp.int32)
    hit_count = (by_source[..., None] == expert_ids).astype(jnp.int32)
    per_token = jnp.sum(hit_count, axis=2)
    before = jnp.cumsum(per_token, axis=1) - per_token
    position = jnp.take_along_axis(before, by_source, axis=2)
    kept_copy = position < CAPACITY
    source_ids = jnp.broadcast_to(jnp.arange(GROUP_DEVS, dtype=jnp.int32)[:, None, None], by_source.shape)
    token_ids = jnp.broadcast_to(jnp.arange(TOKENS, dtype=jnp.int32).reshape(GROUP_DEVS, TOKENS_DEV, 1), by_source.shape)
    slot_table = jnp.zeros((EXPERTS, GROUP_DEVS, CAPACITY), jnp.int32)
    slot_table = slot_table.at[by_source, source_ids, position].set(token_ids, mode="drop")

    def one_expert(operands):
        row_index, gate_mat, up_mat, down_mat = operands
        expert_rows = normed[row_index.reshape(-1)]
        gate_proj = jnp.dot(expert_rows, gate_mat, preferred_element_type=jnp.float32)
        up_proj = jnp.dot(expert_rows, up_mat, preferred_element_type=jnp.float32)
        inner_act = (jax.nn.silu(gate_proj) * up_proj).astype(jnp.bfloat16)
        return jnp.dot(inner_act, down_mat, preferred_element_type=jnp.float32).astype(jnp.bfloat16)

    expert_out = lax.map(one_expert, (slot_table, w_gate, w_up, w_down))
    expert_out = expert_out.reshape(EXPERTS, GROUP_DEVS, CAPACITY, D_MODEL)
    picked = expert_out[by_source, source_ids, jnp.minimum(position, CAPACITY - 1)]
    kept_gates = jnp.where(kept_copy, gate_vals.reshape(GROUP_DEVS, TOKENS_DEV, 2), 0.0)
    mixed_out = hidden.reshape(GROUP_DEVS, TOKENS_DEV, D_MODEL).astype(jnp.float32) + jnp.sum(kept_gates[..., None] * picked.astype(jnp.float32), axis=2)
    return mixed_out.reshape(TOKENS, D_MODEL).astype(jnp.bfloat16)
```

```python
import functools

import jax
import jax.numpy as jnp
from jax import lax
from jax.experimental import pallas as pl
from jax.experimental.pallas import tpu as pltpu
from jax.sharding import PartitionSpec as P

LN_EPS = 1e-5
TOKEN_BLOCK = 256
PIECE = 16


def norm_kernel(x_ref, gamma_ref, beta_ref, out_ref):
    values = x_ref[...].astype(jnp.float32)
    centred = values - jnp.mean(values, axis=-1, keepdims=True)
    variance = jnp.mean(centred * centred, axis=-1, keepdims=True)
    out_ref[...] = (centred * lax.rsqrt(variance + LN_EPS) * gamma_ref[...] + beta_ref[...]).astype(jnp.bfloat16)


def layer_norm(x, gamma, beta, block=256):
    tokens, d = x.shape
    row = pl.BlockSpec((1, d), lambda i: (0, 0))
    tile = pl.BlockSpec((block, d), lambda i: (i, 0))
    return pl.pallas_call(
        norm_kernel,
        grid=(tokens // block,),
        out_shape=jax.ShapeDtypeStruct((tokens, d), jnp.bfloat16),
        in_specs=[tile, row, row],
        out_specs=tile,
        cost_estimate=pl.CostEstimate(flops=10 * tokens * d, bytes_accessed=4 * tokens * d, transcendentals=0),
        name="layer_norm",
    )(x, gamma.reshape(1, d), beta.reshape(1, d))


def sparse_gates(normed, w_router, choice, mask_first, mask_second):
    scores = jnp.dot(normed, w_router, preferred_element_type=jnp.float32)
    expert_ids = jnp.arange(w_router.shape[1], dtype=jnp.int32)

    def gate(mask, pick):
        soft_probs = jax.nn.softmax(jnp.where(mask > 0, scores, -jnp.inf), axis=-1)
        return jnp.sum(jnp.where(pick[:, None] == expert_ids, soft_probs, 0.0), axis=-1)

    return gate(mask_first, choice[:, 0]), gate(mask_second, choice[:, 1])


def mlp_kernel(e, mb, ft, nt, cnt_ref, x_hbm, wg, wu, wd, out_hbm, xv, wgu, wdb, h, ov, xsem, wsem, dsem, osem):
    rows, d = x_hbm.shape
    f = wg.shape[2]
    fsteps, nsteps, sub = f // ft, d // nt, ft // 128
    nblk = lax.div(cnt_ref[0] + (mb - 1), mb)
    nmax = rows // mb

    def gu_copies(i, slot):
        out = []
        for j in range(sub):
            col = pl.multiple_of(i * ft + j * 128, 128)
            out.append(pltpu.make_async_copy(wg.at[e, :, pl.ds(col, 128)], wgu.at[slot, :, pl.ds(2 * j * 128, 128)], wsem.at[slot]))
            out.append(pltpu.make_async_copy(wu.at[e, :, pl.ds(col, 128)], wgu.at[slot, :, pl.ds((2 * j + 1) * 128, 128)], wsem.at[slot]))
        return out

    def wd_copy(i, slot):
        return pltpu.make_async_copy(wd.at[e, :, pl.ds(pl.multiple_of(i * nt, nt), nt)], wdb.at[slot], dsem.at[slot])

    def x_copy(m):
        r = pl.ds(pl.multiple_of(m * mb, mb), mb)
        return pltpu.make_async_copy(x_hbm.at[r], xv.at[r], xsem)

    def out_copy(i, slot):
        return pltpu.make_async_copy(ov.at[slot], out_hbm.at[:, pl.ds(pl.multiple_of(i * nt, nt), nt)], osem.at[slot])

    for c in gu_copies(0, 0):
        c.start()
    def xs(m, _):
        x_copy(m).start()
        return 0
    lax.fori_loop(0, nblk, xs, 0)
    def xw(m, _):
        x_copy(m).wait()
        return 0
    lax.fori_loop(0, nblk, xw, 0)

    def fstep(i, _):
        slot = lax.rem(i, 2)
        @pl.when(i + 1 < fsteps)
        def _():
            for c in gu_copies(i + 1, 1 - slot):
                c.start()
        @pl.when(i + 1 == fsteps)
        def _():
            wd_copy(0, 0).start()
        for c in gu_copies(i, slot):
            c.wait()
        def mstep(m, _):
            r = pl.ds(pl.multiple_of(m * mb, mb), mb)
            xb = xv[r, :]
            for j in range(sub):
                gu = jnp.dot(xb, wgu[slot, :, pl.ds(2 * j * 128, 256)], preferred_element_type=jnp.float32)
                g, u = gu[:, :128], gu[:, 128:]
                h[i * sub + j, r, :] = (g * (1.0 / (1.0 + jnp.exp(-g))) * u).astype(jnp.bfloat16)
            return 0
        lax.fori_loop(0, nblk, mstep, 0)
        return 0
    lax.fori_loop(0, fsteps, fstep, 0)

    def nstep(i, _):
        slot = lax.rem(i, 2)
        @pl.when(i + 1 < nsteps)
        def _():
            wd_copy(i + 1, 1 - slot).start()
        wd_copy(i, slot).wait()
        @pl.when(i >= 2)
        def _():
            out_copy(i - 2, slot).wait()
        def mstep(m, _):
            r = pl.ds(pl.multiple_of(m * mb, mb), mb)
            hb = jnp.concatenate([h[k, r, :] for k in range(f // 128)], axis=1)
            ov[slot, r, :] = jnp.dot(hb, wdb[slot], preferred_element_type=jnp.float32).astype(jnp.bfloat16)
            return 0
        lax.fori_loop(0, nblk, mstep, 0)
        def zstep(m, _):
            r = pl.ds(pl.multiple_of(m * mb, mb), mb)
            ov[slot, r, :] = jnp.zeros((mb, nt), jnp.bfloat16)
            return 0
        lax.fori_loop(nblk, nmax, zstep, 0)
        out_copy(i, slot).start()
        return 0
    lax.fori_loop(0, nsteps, nstep, 0)
    for i in range(max(nsteps - 2, 0), nsteps):
        out_copy(i, i % 2).wait()

def expert_mlp(cnt, x, wg, wu, wd, e, mb=320, ft=640, nt=256):
    rows, d = x.shape
    f = wg.shape[2]
    any_ = pl.BlockSpec(memory_space=pl.ANY)
    return pl.pallas_call(
        functools.partial(mlp_kernel, e, mb, ft, nt),
        out_shape=jax.ShapeDtypeStruct((rows, d), jnp.bfloat16),
        in_specs=[pl.BlockSpec(memory_space=pltpu.SMEM), any_, any_, any_, any_],
        out_specs=any_,
        scratch_shapes=[pltpu.VMEM((rows, d), jnp.bfloat16), pltpu.VMEM((2, d, 2 * ft), jnp.bfloat16),
                        pltpu.VMEM((2, f, nt), jnp.bfloat16), pltpu.VMEM((f // 128, rows, 128), jnp.bfloat16),
                        pltpu.VMEM((2, rows, nt), jnp.bfloat16),
                        pltpu.SemaphoreType.DMA, pltpu.SemaphoreType.DMA((2,)), pltpu.SemaphoreType.DMA((2,)), pltpu.SemaphoreType.DMA((2,))],
        compiler_params=pltpu.CompilerParams(vmem_limit_bytes=60 * 1024 * 1024),
        cost_estimate=pl.CostEstimate(flops=6 * rows * d * f * 3 // 4, bytes_accessed=6 * d * f + 4 * rows * d, transcendentals=0),
        name="expert_mlp",
    )(cnt, x, wg, wu, wd)


def combine_kernel(start_ref, pieces_ref, x_ref, row_ref, gate_ref, *refs):
    sources, out_ref, rows_buf, sem = refs[:-3], refs[-3], refs[-2], refs[-1]
    step, steps = pl.program_id(0), pl.num_programs(0)
    experts = len(sources)
    depth = rows_buf.shape[1]

    def each_piece(block, act):
        slot = lax.rem(block, 2)
        base = jnp.int32(0)
        for e, source in enumerate(sources):
            start, pieces = start_ref[block * experts + e], pieces_ref[block * experts + e]

            def one(p, at, source=source, start=start):
                src = source.at[pl.ds(pl.multiple_of(start + p * PIECE, PIECE), PIECE)]
                dst = rows_buf.at[slot, pl.ds(pl.multiple_of(at, PIECE), PIECE)]
                act(pltpu.make_async_copy(src, dst, sem.at[slot]))
                return at + PIECE

            base = lax.fori_loop(0, pieces, one, base)

    @pl.when(step == 0)
    def _():
        rows_buf[...] = jnp.zeros_like(rows_buf)
        each_piece(step, lambda c: c.start())

    @pl.when(step + 1 < steps)
    def _():
        each_piece(step + 1, lambda c: c.start())

    each_piece(step, lambda c: c.wait())
    slot = lax.rem(step, 2)
    lane = lax.broadcasted_iota(jnp.int32, (x_ref.shape[0], depth), 1)
    first = jnp.where(lane == row_ref[:, 0:1], 1.0, 0.0).astype(jnp.bfloat16)
    second = jnp.where(lane == row_ref[:, 1:2], 1.0, 0.0).astype(jnp.bfloat16)
    width = 256
    for c in range(0, x_ref.shape[1], width):
        cols = slice(c, c + width)
        rows = rows_buf[slot, :, cols]
        y_first = jnp.dot(first, rows, preferred_element_type=jnp.float32)
        y_second = jnp.dot(second, rows, preferred_element_type=jnp.float32)
        mixed = gate_ref[:, 0:1] * y_first + gate_ref[:, 1:2] * y_second
        out_ref[:, cols] = (x_ref[:, cols].astype(jnp.float32) + mixed).astype(jnp.bfloat16)


def combine(x, rows, gates, start, pieces, sources):
    tokens, d = x.shape
    depth = -(-(2 * TOKEN_BLOCK + len(sources) * (2 * PIECE - 2)) // 256) * 256
    tile = pl.BlockSpec((TOKEN_BLOCK, d), lambda i, *_: (i, 0))
    pair = pl.BlockSpec((TOKEN_BLOCK, 2), lambda i, *_: (i, 0))
    return pl.pallas_call(
        combine_kernel,
        grid_spec=pltpu.PrefetchScalarGridSpec(
            num_scalar_prefetch=2,
            grid=(tokens // TOKEN_BLOCK,),
            in_specs=[tile, pair, pair] + [pl.BlockSpec(memory_space=pl.ANY)] * len(sources),
            out_specs=tile,
            scratch_shapes=[pltpu.VMEM((2, depth, d), jnp.bfloat16), pltpu.SemaphoreType.DMA((2,))],
        ),
        out_shape=jax.ShapeDtypeStruct((tokens, d), jnp.bfloat16),
        compiler_params=pltpu.CompilerParams(vmem_limit_bytes=40 * 1024 * 1024),
        cost_estimate=pl.CostEstimate(flops=4 * tokens * depth * d, bytes_accessed=16 * tokens * d, transcendentals=0),
        name="combine",
    )(start, pieces, x, rows, gates, *sources)


def slot_table(slots, slot_count):
    tokens = slots[0].shape[0]
    token = jnp.arange(tokens, dtype=jnp.int32)
    table = 0.0
    for slot in slots:
        high = (slot[:, None] // 128 == jnp.arange(slot_count // 128)).astype(jnp.bfloat16)
        low = slot[:, None] % 128 == jnp.arange(128)
        for part, weight in ((token // 64, 64.0), (token % 64, 1.0)):
            value = jnp.where(low, part[:, None], 0).astype(jnp.bfloat16)
            table += weight * jnp.einsum("th,tl->hl", high, value, preferred_element_type=jnp.float32)
    return table.astype(jnp.int32).reshape(slot_count)


def solution(mesh):
    group_size = mesh.shape["ep"]
    rows_spec = P(("dp", "ep"))

    def exchange(value, distance):
        return lax.ppermute(value, "ep", [(k, k ^ distance) for k in range(group_size)])

    def device_step(hidden, ln_gamma, ln_beta, w_router, w_gate, w_up, w_down, choice, mask_first, mask_second):
        tokens, d = hidden.shape
        local = w_gate.shape[0]
        experts = local * group_size
        capacity = (10 * tokens + 4 * experts - 1) // (4 * experts)
        normed = layer_norm(hidden, ln_gamma, ln_beta)
        rows_of = {0: normed, 1: exchange(normed, 1), 2: exchange(normed, 2)}
        rows_of[3] = exchange(rows_of[2], 1)

        me = lax.axis_index("ep")
        near = choice ^ (me * local)
        ids = jnp.arange(experts, dtype=jnp.int32)
        hit = near[:, :, None] == ids
        per_token = jnp.sum(hit.astype(jnp.int32), axis=1)
        after = jnp.cumsum(per_token, axis=0)
        before = after - per_token
        count = jnp.minimum(after[-1], capacity)
        position = [jnp.sum(jnp.where(hit[:, j], before, 0), axis=1) for j in range(2)]
        slots = [jnp.where(position[j] < capacity, near[:, j] * capacity + position[j], experts * capacity) for j in range(2)]
        table = slot_table(slots, experts * capacity).reshape(group_size, local * capacity)
        message = jnp.concatenate([table, count.reshape(group_size, local)], axis=1)
        inbox = [message[0]] + [exchange(message[r], r) for r in range(1, group_size)]

        results = {}
        for r in range(group_size):
            for i in range(local):
                rows = rows_of[r].at[inbox[r][i * capacity:(i + 1) * capacity]].get(mode="promise_in_bounds")
                y = expert_mlp(inbox[r][local * capacity + i:local * capacity + i + 1], rows, w_gate, w_up, w_down, i)
                results[r * local + i] = exchange(y, r) if r else y

        gates = sparse_gates(normed, w_router, choice, mask_first, mask_second)
        blocks = tokens // TOKEN_BLOCK
        first = jnp.minimum(before.reshape(blocks, TOKEN_BLOCK, experts)[:, 0], capacity)
        last = jnp.concatenate([first[1:], count[None]], axis=0)
        start = first // PIECE * PIECE
        pieces = jnp.where(last > first, (last - start + PIECE - 1) // PIECE, 0)
        offset = (jnp.cumsum(pieces, axis=1) - pieces) * PIECE - start
        offset_rows = jnp.repeat(offset, TOKEN_BLOCK, axis=0, total_repeat_length=tokens)
        rows = []
        for j in range(2):
            at = jnp.sum(jnp.where(hit[:, j], before + offset_rows, 0), axis=1)
            rows.append(jnp.where(position[j] < capacity, at, -1))
        return combine(hidden, jnp.stack(rows, axis=1), jnp.stack(gates, axis=1), start.reshape(-1), pieces.reshape(-1),
                       [results[k] for k in range(experts)])

    return jax.shard_map(device_step, mesh=mesh,
                         in_specs=(rows_spec, P(), P(), P(), P("ep"), P("ep"), P("ep"), rows_spec, rows_spec, rows_spec),
                         out_specs=rows_spec, check_vma=False)
```

```python
import functools

import jax
import jax.numpy as jnp
from jax import lax
from jax.experimental import pallas as pl
from jax.experimental.pallas import tpu as pltpu
from jax.sharding import PartitionSpec as P


LN_EPS = 1e-5
TOKEN_BLOCK = 256
PIECE = 16
PACK_ROWS = 96
MLP_ROWS = 320


def norm_kernel(x_ref, gamma_ref, beta_ref, out_ref):
    values = x_ref[...].astype(jnp.float32)
    centred = values - jnp.mean(values, axis=-1, keepdims=True)
    variance = jnp.mean(centred * centred, axis=-1, keepdims=True)
    out_ref[...] = (centred * lax.rsqrt(variance + LN_EPS) * gamma_ref[...] + beta_ref[...]).astype(jnp.bfloat16)


def layer_norm(x, gamma, beta, block=512):
    tokens, d = x.shape
    row = pl.BlockSpec((1, d), lambda i: (0, 0))
    tile = pl.BlockSpec((block, d), lambda i: (i, 0))
    return pl.pallas_call(
        norm_kernel,
        grid=(tokens // block,),
        out_shape=jax.ShapeDtypeStruct((tokens, d), jnp.bfloat16),
        in_specs=[tile, row, row],
        out_specs=tile,
        compiler_params=pltpu.CompilerParams(vmem_limit_bytes=48 * 1024 * 1024),
        cost_estimate=pl.CostEstimate(flops=10 * tokens * d, bytes_accessed=4 * tokens * d, transcendentals=0),
        name="layer_norm",
    )(x, gamma.reshape(1, d), beta.reshape(1, d))


def sparse_gates(normed, w_router, choice, mask_first, mask_second):
    scores = jnp.dot(normed, w_router, preferred_element_type=jnp.float32)
    expert_ids = jnp.arange(w_router.shape[1], dtype=jnp.int32)

    def gate(mask, pick):
        soft_probs = jax.nn.softmax(jnp.where(mask > 0, scores, -jnp.inf), axis=-1)
        return jnp.sum(jnp.where(pick[:, None] == expert_ids, soft_probs, 0.0), axis=-1)

    return gate(mask_first, choice[:, 0]), gate(mask_second, choice[:, 1])


def pack_kernel(start_ref, pieces_ref, slot_ref, rows_ref, out_ref):
    block = pl.program_id(0)
    local, depth = out_ref.shape[0], out_ref.shape[1]
    tokens = rows_ref.shape[0]

    @pl.when(block == 0)
    def _():
        out_ref[...] = jnp.zeros_like(out_ref)

    pieces = pieces_ref[block * local]
    for i in range(1, local):
        pieces = jnp.maximum(pieces, pieces_ref[block * local + i])
    line = lax.broadcasted_iota(jnp.int32, (PACK_ROWS, tokens), 0)

    def one(p, _):
        at, picks = [], []
        for i in range(local):
            first = jnp.minimum(start_ref[block * local + i] + p * PACK_ROWS, depth - PACK_ROWS)
            at.append(pl.ds(pl.multiple_of(first, PIECE), PACK_ROWS))
            picks.append(jnp.where(slot_ref[i:i + 1, :] - first == line, 1.0, 0.0).astype(jnp.bfloat16))
        pick = jnp.concatenate(picks, axis=0)
        width = 256
        for c in range(0, rows_ref.shape[1], width):
            cols = slice(c, c + width)
            packed = jnp.dot(pick, rows_ref[:, cols], preferred_element_type=jnp.float32)
            for i in range(local):
                part = packed[i * PACK_ROWS:(i + 1) * PACK_ROWS]
                out_ref[i, at[i], cols] = (out_ref[i, at[i], cols].astype(jnp.float32) + part).astype(jnp.bfloat16)
        return 0

    lax.fori_loop(0, pieces, one, 0)


def pack_rows(rows, slot, start, pieces, capacity):
    tokens, d = rows.shape
    local = slot.shape[0]
    depth = capacity + PACK_ROWS
    return pl.pallas_call(
        pack_kernel,
        grid_spec=pltpu.PrefetchScalarGridSpec(
            num_scalar_prefetch=2,
            grid=(tokens // TOKEN_BLOCK,),
            in_specs=[pl.BlockSpec((local, TOKEN_BLOCK), lambda b, *_: (0, b)), pl.BlockSpec((TOKEN_BLOCK, d), lambda b, *_: (b, 0))],
            out_specs=pl.BlockSpec((local, depth, d), lambda b, *_: (0, 0, 0)),
        ),
        out_shape=jax.ShapeDtypeStruct((local, depth, d), jnp.bfloat16),
        compiler_params=pltpu.CompilerParams(vmem_limit_bytes=48 * 1024 * 1024),
        cost_estimate=pl.CostEstimate(flops=4 * tokens * d * PACK_ROWS, bytes_accessed=4 * tokens * d, transcendentals=0),
        name="pack_rows",
    )(start, pieces, slot, rows)


def mlp_kernel(e, origin, mb, ft, nt, cnt_ref, x_hbm, wg, wu, wd, prior, out_hbm, xv, wbuf, h, ov, xsem, wsem, osem):
    rows, d = out_hbm.shape
    f = wg.shape[2]
    fsteps, nsteps, sub = f // ft, d // nt, ft // 128
    panels = -(-f // d)
    nblk = lax.div(jnp.clip(cnt_ref[e] - origin, 0, rows) + (mb - 1), mb)

    def gu_copies(i, slot):
        out = []
        for j in range(sub):
            col = pl.ds(pl.multiple_of(i * ft + j * 128, 128), 128)
            out.append(pltpu.make_async_copy(wg.at[e, :, col], wbuf.at[slot, :, pl.ds(2 * j * 128, 128)], wsem.at[slot]))
            out.append(pltpu.make_async_copy(wu.at[e, :, col], wbuf.at[slot, :, pl.ds((2 * j + 1) * 128, 128)], wsem.at[slot]))
        return out

    def wd_copies(i, slot):
        out = []
        for k in range(panels):
            lines = min(d, f - k * d)
            col = pl.ds(pl.multiple_of(i * nt, nt), nt)
            out.append(pltpu.make_async_copy(wd.at[e, pl.ds(k * d, lines), col], wbuf.at[slot, pl.ds(0, lines), pl.ds(k * nt, nt)], wsem.at[slot]))
        return out

    def x_copy(m):
        at = pl.multiple_of(m * mb, mb)
        return pltpu.make_async_copy(x_hbm.at[e, pl.ds(at + origin, mb)], xv.at[pl.ds(at, mb)], xsem)

    def out_copy(i, slot):
        return pltpu.make_async_copy(ov.at[slot], out_hbm.at[:, pl.ds(pl.multiple_of(i * nt, nt), nt)], osem.at[slot])

    def each(copies, act):
        for c in copies:
            act(c)

    def loop(lo, hi, body):
        def step(m, _):
            body(m)
            return 0
        lax.fori_loop(lo, hi, step, 0)

    each(gu_copies(0, 0), lambda c: c.start())
    loop(0, nblk, lambda m: x_copy(m).start())
    loop(0, nblk, lambda m: x_copy(m).wait())

    def fstep(i):
        slot = lax.rem(i, 2)

        @pl.when(i + 1 < fsteps)
        def _():
            each(gu_copies(i + 1, 1 - slot), lambda c: c.start())

        @pl.when(i + 1 == fsteps)
        def _():
            each(wd_copies(0, fsteps % 2), lambda c: c.start())

        each(gu_copies(i, slot), lambda c: c.wait())

        def mstep(m):
            r = pl.ds(pl.multiple_of(m * mb, mb), mb)
            xb = xv[r, :]
            for j in range(sub):
                gu = jnp.dot(xb, wbuf[slot, :, pl.ds(2 * j * 128, 256)], preferred_element_type=jnp.float32)
                g, u = gu[:, :128], gu[:, 128:]
                h[i * sub + j, r, :] = (g * (1.0 / (1.0 + jnp.exp(-g))) * u).astype(jnp.bfloat16)

        loop(0, nblk, mstep)

    loop(0, fsteps, fstep)

    def nstep(i):
        slot, oslot = lax.rem(i + fsteps, 2), lax.rem(i, 2)

        @pl.when(i + 1 < nsteps)
        def _():
            each(wd_copies(i + 1, 1 - slot), lambda c: c.start())

        each(wd_copies(i, slot), lambda c: c.wait())

        @pl.when(i >= 2)
        def _():
            out_copy(i - 2, oslot).wait()

        def mstep(m):
            r = pl.ds(pl.multiple_of(m * mb, mb), mb)
            width = 256
            parts = []
            for k in range(panels):
                lines = min(d, f - k * d)
                parts.append(jnp.concatenate([h[q, r, :] for q in range(k * d // 128, (k * d + lines) // 128)], axis=1))
            for c in range(0, nt, width):
                acc = 0.0
                for k in range(panels):
                    lines = min(d, f - k * d)
                    acc += jnp.dot(parts[k], wbuf[slot, pl.ds(0, lines), pl.ds(k * nt + c, width)], preferred_element_type=jnp.float32)
                ov[oslot, r, pl.ds(c, width)] = acc.astype(jnp.bfloat16)

        loop(0, nblk, mstep)

        def zstep(m):
            ov[oslot, pl.ds(pl.multiple_of(m * mb, mb), mb), :] = jnp.zeros((mb, nt), jnp.bfloat16)

        loop(nblk, rows // mb, zstep)
        out_copy(i, oslot).start()

    loop(0, nsteps, nstep)
    for i in range(max(nsteps - 2, 0), nsteps):
        out_copy(i, i % 2).wait()


def expert_mlp(cnt, x, wg, wu, wd, prior, e, origin, rows, mb=MLP_ROWS):
    d, f = wg.shape[1:]
    ft = 1152 if f % 1152 == 0 else 640
    nt = 768 if d % 768 == 0 else 256
    any_ = pl.BlockSpec(memory_space=pl.ANY)
    return pl.pallas_call(
        functools.partial(mlp_kernel, e, origin, mb, ft, nt),
        out_shape=jax.ShapeDtypeStruct((rows, d), jnp.bfloat16),
        in_specs=[pl.BlockSpec(memory_space=pltpu.SMEM)] + [any_] * 5,
        out_specs=any_,
        scratch_shapes=[pltpu.VMEM((rows, d), jnp.bfloat16), pltpu.VMEM((2, d, 2 * ft), jnp.bfloat16),
                        pltpu.VMEM((f // 128, rows, 128), jnp.bfloat16), pltpu.VMEM((2, rows, nt), jnp.bfloat16),
                        pltpu.SemaphoreType.DMA, pltpu.SemaphoreType.DMA((2,)), pltpu.SemaphoreType.DMA((2,))],
        compiler_params=pltpu.CompilerParams(vmem_limit_bytes=60 * 1024 * 1024),
        cost_estimate=pl.CostEstimate(flops=6 * rows * d * f, bytes_accessed=6 * d * f + 4 * rows * d, transcendentals=0),
        name="expert_mlp",
    )(cnt, x, wg, wu, wd, prior)


def combine_kernel(parts, start_ref, pieces_ref, x_ref, row_ref, gate_ref, *refs):
    refs, out_ref, rows_buf, sem = list(refs[:-3]), refs[-3], refs[-2], refs[-1]
    sources = [[refs.pop(0) for _ in range(n)] for n in parts]
    step, steps = pl.program_id(0), pl.num_programs(0)
    experts = len(sources)
    depth = rows_buf.shape[1]

    def each_piece(block, act):
        slot = lax.rem(block, 2)
        base = jnp.int32(0)
        for e, source in enumerate(sources):
            start, pieces = start_ref[block * experts + e], pieces_ref[block * experts + e]
            end = start + pieces * PIECE
            for q, part in enumerate(source):
                size = part.shape[0]
                low, high = jnp.clip(start - q * size, 0, size), jnp.clip(end - q * size, 0, size)

                def one(p, at, part=part, low=low):
                    src = part.at[pl.ds(pl.multiple_of(low + p * PIECE, PIECE), PIECE)]
                    dst = rows_buf.at[slot, pl.ds(pl.multiple_of(at, PIECE), PIECE)]
                    act(pltpu.make_async_copy(src, dst, sem.at[slot]))
                    return at + PIECE

                base = lax.fori_loop(0, lax.div(high - low, PIECE), one, base)

    @pl.when(step == 0)
    def _():
        rows_buf[...] = jnp.zeros_like(rows_buf)
        each_piece(step, lambda c: c.start())

    @pl.when(step + 1 < steps)
    def _():
        each_piece(step + 1, lambda c: c.start())

    each_piece(step, lambda c: c.wait())
    slot = lax.rem(step, 2)
    lane = lax.broadcasted_iota(jnp.int32, (x_ref.shape[0], depth), 1)
    first = jnp.where(lane == row_ref[:, 0:1], 1.0, 0.0).astype(jnp.bfloat16)
    second = jnp.where(lane == row_ref[:, 1:2], 1.0, 0.0).astype(jnp.bfloat16)
    width = 256
    for c in range(0, x_ref.shape[1], width):
        cols = slice(c, c + width)
        rows = rows_buf[slot, :, cols]
        y_first = jnp.dot(first, rows, preferred_element_type=jnp.float32)
        y_second = jnp.dot(second, rows, preferred_element_type=jnp.float32)
        mixed = gate_ref[:, 0:1] * y_first + gate_ref[:, 1:2] * y_second
        out_ref[:, cols] = (x_ref[:, cols].astype(jnp.float32) + mixed).astype(jnp.bfloat16)


def combine(x, rows, gates, start, pieces, sources):
    tokens, d = x.shape
    depth = -(-(2 * TOKEN_BLOCK + len(sources) * (2 * PIECE - 2)) // 256) * 256
    tile = pl.BlockSpec((TOKEN_BLOCK, d), lambda i, *_: (i, 0))
    pair = pl.BlockSpec((TOKEN_BLOCK, 2), lambda i, *_: (i, 0))
    return pl.pallas_call(
        functools.partial(combine_kernel, [len(s) for s in sources]),
        grid_spec=pltpu.PrefetchScalarGridSpec(
            num_scalar_prefetch=2,
            grid=(tokens // TOKEN_BLOCK,),
            in_specs=[tile, pair, pair] + [pl.BlockSpec(memory_space=pl.ANY)] * sum(map(len, sources)),
            out_specs=tile,
            scratch_shapes=[pltpu.VMEM((2, depth, d), jnp.bfloat16), pltpu.SemaphoreType.DMA((2,))],
        ),
        out_shape=jax.ShapeDtypeStruct((tokens, d), jnp.bfloat16),
        compiler_params=pltpu.CompilerParams(vmem_limit_bytes=40 * 1024 * 1024),
        cost_estimate=pl.CostEstimate(flops=4 * tokens * depth * d, bytes_accessed=16 * tokens * d, transcendentals=0),
        name="combine",
    )(start, pieces, x, rows, gates, *sum(sources, []))


def solution(mesh):
    group_size = mesh.shape["ep"]
    rows_spec = P(("dp", "ep"))

    def exchange(value, distance):
        return lax.ppermute(value, "ep", [(k, k ^ distance) for k in range(group_size)])

    def device_step(hidden, ln_gamma, ln_beta, w_router, w_gate, w_up, w_down, choice, mask_first, mask_second):
        tokens, d = hidden.shape
        local = w_gate.shape[0]
        experts = local * group_size
        capacity = (10 * tokens + 4 * experts - 1) // (4 * experts)
        blocks = tokens // TOKEN_BLOCK
        choices = [choice.T] + [exchange(choice.T, r) for r in range(1, group_size)]
        ln_gamma, choices = lax.optimization_barrier((ln_gamma, choices))
        normed = layer_norm(hidden, ln_gamma, ln_beta)
        rows_of = {0: normed, 1: exchange(normed, 1), 2: exchange(normed, 2)}
        rows_of[3] = exchange(rows_of[2], 1)

        me = lax.axis_index("ep")
        here = me * local + jnp.arange(local, dtype=jnp.int32)
        near = choice.T ^ (me * local)
        ids = jnp.arange(experts, dtype=jnp.int32)
        hit = [jnp.any(c[:, None, :] == here[:, None], axis=0) for c in choices] + [jnp.any(near[:, None, :] == ids[:, None], axis=0)]
        hit = jnp.concatenate(hit, axis=0).astype(jnp.int32)
        after = jnp.cumsum(hit, axis=1)
        before = after - hit
        count = jnp.minimum(after[:, -1], capacity)
        slot = jnp.where((hit > 0) & (before < capacity), before, -1)
        first = jnp.minimum(before[:, ::TOKEN_BLOCK], capacity)
        last = jnp.concatenate([first[:, 1:], count[:, None]], axis=1)
        start = first // PIECE * PIECE
        length = jnp.where(last > first, last - start, 0)

        pack_pieces = (length[:experts] + PACK_ROWS - 1) // PACK_ROWS
        results = {}
        order = [(0, 0, 1), (1, 0, 1), (1, 1, 1), (0, 1, 1)] + [(r, i, 2) for r in (2, 3) for i in range(local)]
        packed = {}
        y = normed
        for r, i, parts in order:
            own = slice(r * local, (r + 1) * local)
            if r not in packed:
                packed[r] = pack_rows(rows_of[r], slot[own], start[own].T.reshape(-1), pack_pieces[own].T.reshape(-1), capacity)
            size = capacity // parts
            for q in range(parts):
                y = expert_mlp(count[own], packed[r], w_gate, w_up, w_down, y, i, q * size, size)
                results[r, i, q] = exchange(y, r) if r else y

        gates = sparse_gates(normed, w_router, choice, mask_first, mask_second)
        start, length, before, slot = start[experts:], length[experts:], before[experts:], slot[experts:]
        pieces = (length + PIECE - 1) // PIECE
        offset = (jnp.cumsum(pieces, axis=0) - pieces) * PIECE - start
        line = before + jnp.broadcast_to(offset[:, :, None], (experts, blocks, TOKEN_BLOCK)).reshape(experts, tokens)
        line = jnp.where(slot >= 0, line, -1)
        rows = [jnp.sum(jnp.where(near[j] == ids[:, None], line, 0), axis=0) for j in range(2)]
        sources = [[results[r, i, q] for q in range(2) if (r, i, q) in results] for r in range(group_size) for i in range(local)]
        return combine(hidden, jnp.stack(rows, axis=1), jnp.stack(gates, axis=1), start.T.reshape(-1), pieces.T.reshape(-1), sources)

    return jax.shard_map(device_step, mesh=mesh,
                         in_specs=(rows_spec, P(), P(), P(), P("ep"), P("ep"), P("ep"), rows_spec, rows_spec, rows_spec),
                         out_specs=rows_spec, check_vma=False)
```

```python
import functools

import jax
import jax.numpy as jnp
from jax import lax
from jax.experimental import pallas as pl
from jax.experimental.pallas import tpu as pltpu
from jax.sharding import PartitionSpec as P


LN_EPS = 1e-5
TOKEN_BLOCK = 256
PIECE = 16
WIDE_PIECE = 64
PACK_ROWS = 96
MLP_ROWS = 320


def norm_kernel(x_ref, gamma_ref, beta_ref, out_ref):
    values = x_ref[...].astype(jnp.float32)
    centred = values - jnp.mean(values, axis=-1, keepdims=True)
    variance = jnp.mean(centred * centred, axis=-1, keepdims=True)
    out_ref[...] = (centred * lax.rsqrt(variance + LN_EPS) * gamma_ref[...] + beta_ref[...]).astype(jnp.bfloat16)


def layer_norm(x, gamma, beta, block=512):
    tokens, d = x.shape
    row = pl.BlockSpec((1, d), lambda i: (0, 0))
    tile = pl.BlockSpec((block, d), lambda i: (i, 0))
    return pl.pallas_call(
        norm_kernel,
        grid=(tokens // block,),
        out_shape=jax.ShapeDtypeStruct((tokens, d), jnp.bfloat16),
        in_specs=[tile, row, row],
        out_specs=tile,
        compiler_params=pltpu.CompilerParams(vmem_limit_bytes=48 * 1024 * 1024),
        cost_estimate=pl.CostEstimate(flops=10 * tokens * d, bytes_accessed=4 * tokens * d, transcendentals=0),
        name="layer_norm",
    )(x, gamma.reshape(1, d), beta.reshape(1, d))


def sparse_gates(normed, w_router, choice, mask_first, mask_second):
    scores = jnp.dot(normed, w_router, preferred_element_type=jnp.float32)
    expert_ids = jnp.arange(w_router.shape[1], dtype=jnp.int32)

    def gate(mask, pick):
        soft_probs = jax.nn.softmax(jnp.where(mask > 0, scores, -jnp.inf), axis=-1)
        return jnp.sum(jnp.where(pick[:, None] == expert_ids, soft_probs, 0.0), axis=-1)

    return gate(mask_first, choice[:, 0]), gate(mask_second, choice[:, 1])


def pack_kernel(start_ref, pieces_ref, slot_ref, rows_ref, out_ref):
    block = pl.program_id(0)
    local, depth = out_ref.shape[0], out_ref.shape[1]
    tokens = rows_ref.shape[0]

    @pl.when(block == 0)
    def _():
        out_ref[...] = jnp.zeros_like(out_ref)

    pieces = pieces_ref[block * local]
    for i in range(1, local):
        pieces = jnp.maximum(pieces, pieces_ref[block * local + i])
    line = lax.broadcasted_iota(jnp.int32, (PACK_ROWS, tokens), 0)

    def one(p, _):
        at, picks = [], []
        for i in range(local):
            first = jnp.minimum(start_ref[block * local + i] + p * PACK_ROWS, depth - PACK_ROWS)
            at.append(pl.ds(pl.multiple_of(first, PIECE), PACK_ROWS))
            picks.append(jnp.where(slot_ref[i:i + 1, :] - first == line, 1.0, 0.0).astype(jnp.bfloat16))
        pick = jnp.concatenate(picks, axis=0)
        width = 256
        for c in range(0, rows_ref.shape[1], width):
            cols = slice(c, c + width)
            packed = jnp.dot(pick, rows_ref[:, cols], preferred_element_type=jnp.float32)
            for i in range(local):
                part = packed[i * PACK_ROWS:(i + 1) * PACK_ROWS]
                out_ref[i, at[i], cols] = (out_ref[i, at[i], cols].astype(jnp.float32) + part).astype(jnp.bfloat16)
        return 0

    lax.fori_loop(0, pieces, one, 0)


def pack_rows(rows, slot, start, pieces, capacity):
    tokens, d = rows.shape
    local = slot.shape[0]
    depth = capacity + PACK_ROWS
    return pl.pallas_call(
        pack_kernel,
        grid_spec=pltpu.PrefetchScalarGridSpec(
            num_scalar_prefetch=2,
            grid=(tokens // TOKEN_BLOCK,),
            in_specs=[pl.BlockSpec((local, TOKEN_BLOCK), lambda b, *_: (0, b)), pl.BlockSpec((TOKEN_BLOCK, d), lambda b, *_: (b, 0))],
            out_specs=pl.BlockSpec((local, depth, d), lambda b, *_: (0, 0, 0)),
        ),
        out_shape=jax.ShapeDtypeStruct((local, depth, d), jnp.bfloat16),
        compiler_params=pltpu.CompilerParams(vmem_limit_bytes=48 * 1024 * 1024),
        cost_estimate=pl.CostEstimate(flops=4 * tokens * d * PACK_ROWS, bytes_accessed=4 * tokens * d, transcendentals=0),
        name="pack_rows",
    )(start, pieces, slot, rows)


def mlp_kernel(e, origin, mb, ft, nt, cnt_ref, x_hbm, wg, wu, wd, prior, out_hbm, xv, wbuf, h, ov, xsem, wsem, osem):
    rows, d = out_hbm.shape
    f = wg.shape[2]
    fsteps, nsteps, sub = f // ft, d // nt, ft // 128
    panels = -(-f // d)
    nblk = jnp.maximum(lax.div(jnp.clip(cnt_ref[e] - origin, 0, rows) + (mb - 1), mb), 1)

    def gu_pair(i, slot, j):
        col = pl.ds(pl.multiple_of(i * ft + j * 128, 128), 128)
        gate = wbuf.at[slot, :, pl.ds(pl.multiple_of(2 * j * 128, 128), 128)]
        up = wbuf.at[slot, :, pl.ds(pl.multiple_of((2 * j + 1) * 128, 128), 128)]
        sem = wsem.at[slot, j]
        return [pltpu.make_async_copy(wg.at[e, :, col], gate, sem), pltpu.make_async_copy(wu.at[e, :, col], up, sem)]

    def gu_copies(i, slot):
        return [c for j in range(sub) for c in gu_pair(i, slot, j)]

    def wd_copies(i, slot):
        out = []
        for k in range(panels):
            lines = min(d, f - k * d)
            col = pl.ds(pl.multiple_of(i * nt, nt), nt)
            out.append(pltpu.make_async_copy(wd.at[e, pl.ds(k * d, lines), col], wbuf.at[slot, pl.ds(0, lines), pl.ds(k * nt, nt)], wsem.at[slot, 0]))
        return out

    def x_copy(m):
        at = pl.multiple_of(m * mb, mb)
        return pltpu.make_async_copy(x_hbm.at[e, pl.ds(at + origin, mb)], xv.at[pl.ds(at, mb)], xsem.at[m])

    def out_copy(i, slot):
        return pltpu.make_async_copy(ov.at[slot], out_hbm.at[:, pl.ds(pl.multiple_of(i * nt, nt), nt)], osem.at[slot])

    def each(copies, act):
        for c in copies:
            act(c)

    def loop(lo, hi, body):
        def step(m, _):
            body(m)
            return 0
        lax.fori_loop(lo, hi, step, 0)

    def gate_up(i, slot, m, j):
        both = pl.ds(pl.multiple_of(2 * j * 128, 256), 256)
        r = pl.ds(pl.multiple_of(m * mb, mb), mb)
        gu = jnp.dot(xv[r, :], wbuf[slot, :, both], preferred_element_type=jnp.float32)
        g, u = gu[:, :128], gu[:, 128:]
        h[i * sub + j, r, :] = (g * (1.0 / (1.0 + jnp.exp(-g))) * u).astype(jnp.bfloat16)

    x_copy(0).start()
    each(gu_copies(0, 0), lambda c: c.start())
    loop(1, nblk, lambda m: x_copy(m).start())
    x_copy(0).wait()

    def stream(j):
        each(gu_pair(0, 0, j), lambda c: c.wait())
        each(gu_pair(1, 1, j), lambda c: c.start())
        gate_up(0, 0, 0, j)

    loop(0, sub, stream)
    loop(1, nblk, lambda m: x_copy(m).wait())

    def fstep(i):
        slot = lax.rem(i, 2)

        @pl.when((i > 0) & (i + 1 < fsteps))
        def _():
            each(gu_copies(i + 1, 1 - slot), lambda c: c.start())

        @pl.when(i + 1 == fsteps)
        def _():
            each(wd_copies(0, fsteps % 2), lambda c: c.start())

        @pl.when(i > 0)
        def _():
            each(gu_copies(i, slot), lambda c: c.wait())

        def mstep(m):
            for j in range(sub):
                gate_up(i, slot, m, j)

        loop(jnp.where(i > 0, 0, 1), nblk, mstep)

    loop(0, fsteps, fstep)

    def nstep(i):
        slot, oslot = lax.rem(i + fsteps, 2), lax.rem(i, 2)

        @pl.when(i + 1 < nsteps)
        def _():
            each(wd_copies(i + 1, 1 - slot), lambda c: c.start())

        each(wd_copies(i, slot), lambda c: c.wait())

        @pl.when(i >= 2)
        def _():
            out_copy(i - 2, oslot).wait()

        def mstep(m):
            r = pl.ds(pl.multiple_of(m * mb, mb), mb)
            width = 256
            parts = []
            for k in range(panels):
                lines = min(d, f - k * d)
                parts.append(jnp.concatenate([h[q, r, :] for q in range(k * d // 128, (k * d + lines) // 128)], axis=1))
            for c in range(0, nt, width):
                acc = 0.0
                for k in range(panels):
                    lines = min(d, f - k * d)
                    acc += jnp.dot(parts[k], wbuf[slot, pl.ds(0, lines), pl.ds(k * nt + c, width)], preferred_element_type=jnp.float32)
                ov[oslot, r, pl.ds(c, width)] = acc.astype(jnp.bfloat16)

        loop(0, nblk, mstep)

        def zstep(m):
            ov[oslot, pl.ds(pl.multiple_of(m * mb, mb), mb), :] = jnp.zeros((mb, nt), jnp.bfloat16)

        loop(nblk, rows // mb, zstep)
        out_copy(i, oslot).start()

    loop(0, nsteps, nstep)
    for i in range(max(nsteps - 2, 0), nsteps):
        out_copy(i, i % 2).wait()


def expert_mlp(cnt, x, wg, wu, wd, prior, e, origin, rows, mb=MLP_ROWS):
    d, f = wg.shape[1:]
    ft = 1152 if f % 1152 == 0 else 640
    nt = 768 if d % 768 == 0 else 256
    any_ = pl.BlockSpec(memory_space=pl.ANY)
    return pl.pallas_call(
        functools.partial(mlp_kernel, e, origin, mb, ft, nt),
        out_shape=jax.ShapeDtypeStruct((rows, d), jnp.bfloat16),
        in_specs=[pl.BlockSpec(memory_space=pltpu.SMEM)] + [any_] * 5,
        out_specs=any_,
        scratch_shapes=[pltpu.VMEM((rows, d), jnp.bfloat16), pltpu.VMEM((2, d, 2 * ft), jnp.bfloat16),
                        pltpu.VMEM((f // 128, rows, 128), jnp.bfloat16), pltpu.VMEM((2, rows, nt), jnp.bfloat16),
                        pltpu.SemaphoreType.DMA((rows // mb,)), pltpu.SemaphoreType.DMA((2, ft // 128)), pltpu.SemaphoreType.DMA((2,))],
        compiler_params=pltpu.CompilerParams(vmem_limit_bytes=60 * 1024 * 1024),
        cost_estimate=pl.CostEstimate(flops=6 * rows * d * f, bytes_accessed=6 * d * f + 4 * rows * d, transcendentals=0),
        name="expert_mlp",
    )(cnt, x, wg, wu, wd, prior)


def combine_kernel(parts, tail, split_ref, start_ref, pieces_ref, x_ref, row_ref, gate_ref, *refs):
    refs, out_ref, rows_buf, sem = list(refs[:-3]), refs[-3], refs[-2], refs[-1]
    sources = [[refs.pop(0) for _ in range(n)] for n in parts]
    step, steps = pl.program_id(0), pl.num_programs(0)
    lo, hi = (split_ref[0], steps) if tail else (0, split_ref[0])
    experts = len(sources)
    depth = rows_buf.shape[1]

    def each_piece(block, act):
        slot = lax.rem(block, 2)
        base = jnp.int32(0)
        for e, source in enumerate(sources):
            start, pieces = start_ref[block * experts + e], pieces_ref[block * experts + e]
            end, offset = start + pieces * PIECE, 0
            for part in source:
                size = part.shape[0]
                low, high = jnp.clip(start - offset, 0, size), jnp.clip(end - offset, 0, size)
                offset += size
                wide = lax.div(high - low, WIDE_PIECE)

                def one(rows, p, at, part=part, low=low):
                    src = part.at[pl.ds(pl.multiple_of(low + (at - p), PIECE), rows)]
                    dst = rows_buf.at[slot, pl.ds(pl.multiple_of(at, PIECE), rows)]
                    act(pltpu.make_async_copy(src, dst, sem.at[slot]))
                    return at + rows

                first = base
                base = lax.fori_loop(0, wide, lambda p, at: one(WIDE_PIECE, first, at), base)
                base = lax.fori_loop(0, lax.div(high - low - wide * WIDE_PIECE, PIECE), lambda p, at: one(PIECE, first, at), base)

    @pl.when(step == 0)
    def _():
        rows_buf[...] = jnp.zeros_like(rows_buf)

    @pl.when((step == lo) & (step < hi))
    def _():
        each_piece(step, lambda c: c.start())

    @pl.when((step >= lo) & (step + 1 < hi))
    def _():
        each_piece(step + 1, lambda c: c.start())

    @pl.when((step >= lo) & (step < hi))
    def _():
        each_piece(step, lambda c: c.wait())
        slot = lax.rem(step, 2)
        lane = lax.broadcasted_iota(jnp.int32, (x_ref.shape[0], depth), 1)
        first = jnp.where(lane == row_ref[:, 0:1], 1.0, 0.0).astype(jnp.bfloat16)
        second = jnp.where(lane == row_ref[:, 1:2], 1.0, 0.0).astype(jnp.bfloat16)
        width = 256
        for c in range(0, x_ref.shape[1], width):
            cols = slice(c, c + width)
            rows = rows_buf[slot, :, cols]
            y_first = jnp.dot(first, rows, preferred_element_type=jnp.float32)
            y_second = jnp.dot(second, rows, preferred_element_type=jnp.float32)
            mixed = gate_ref[:, 0:1] * y_first + gate_ref[:, 1:2] * y_second
            out_ref[:, cols] = (x_ref[:, cols].astype(jnp.float32) + mixed).astype(jnp.bfloat16)


def combine(x, rows, gates, split, start, pieces, sources, earlier=None):
    tokens, d = x.shape
    depth = -(-(2 * TOKEN_BLOCK + len(sources) * (2 * PIECE - 2)) // 256) * 256
    tail = earlier is not None
    block = (lambda i, s, *_: (jnp.maximum(i, s[0]), 0)) if tail else (lambda i, s, *_: (jnp.clip(i, 0, jnp.maximum(s[0] - 1, 0)), 0))
    tile = pl.BlockSpec((TOKEN_BLOCK, d), block)
    pair = pl.BlockSpec((TOKEN_BLOCK, 2), block)
    flat = sum(sources, []) + ([earlier] if tail else [])
    return pl.pallas_call(
        functools.partial(combine_kernel, [len(s) for s in sources], tail),
        grid_spec=pltpu.PrefetchScalarGridSpec(
            num_scalar_prefetch=3,
            grid=(tokens // TOKEN_BLOCK,),
            in_specs=[tile, pair, pair] + [pl.BlockSpec(memory_space=pl.ANY)] * len(flat),
            out_specs=tile,
            scratch_shapes=[pltpu.VMEM((2, depth, d), jnp.bfloat16), pltpu.SemaphoreType.DMA((2,))],
        ),
        out_shape=jax.ShapeDtypeStruct((tokens, d), jnp.bfloat16),
        input_output_aliases={len(flat) + 5: 0} if tail else {},
        compiler_params=pltpu.CompilerParams(vmem_limit_bytes=40 * 1024 * 1024),
        cost_estimate=pl.CostEstimate(flops=4 * tokens * depth * d, bytes_accessed=16 * tokens * d, transcendentals=0),
        name="combine",
    )(split, start, pieces, x, rows, gates, *flat)


def solution(mesh):
    group_size = mesh.shape["ep"]
    rows_spec = P(("dp", "ep"))

    def exchange(value, distance):
        return lax.ppermute(value, "ep", [(k, k ^ distance) for k in range(group_size)])

    def device_step(hidden, ln_gamma, ln_beta, w_router, w_gate, w_up, w_down, choice, mask_first, mask_second):
        tokens, d = hidden.shape
        local = w_gate.shape[0]
        experts = local * group_size
        capacity = (10 * tokens + 4 * experts - 1) // (4 * experts)
        blocks = tokens // TOKEN_BLOCK
        choices = [choice.T] + [exchange(choice.T, r) for r in range(1, group_size)]
        ln_gamma, choices = lax.optimization_barrier((ln_gamma, choices))
        normed = layer_norm(hidden, ln_gamma, ln_beta)
        rows_of = {0: normed, 1: exchange(normed, 1), 2: exchange(normed, 2)}
        rows_of[3] = exchange(rows_of[2], 1)

        me = lax.axis_index("ep")
        here = me * local + jnp.arange(local, dtype=jnp.int32)
        near = choice.T ^ (me * local)
        ids = jnp.arange(experts, dtype=jnp.int32)
        hit = [jnp.any(c[:, None, :] == here[:, None], axis=0) for c in choices] + [jnp.any(near[:, None, :] == ids[:, None], axis=0)]
        hit = jnp.concatenate(hit, axis=0).astype(jnp.int32)
        after = jnp.cumsum(hit, axis=1)
        before = after - hit
        count = jnp.minimum(after[:, -1], capacity)
        slot = jnp.where((hit > 0) & (before < capacity), before, -1)
        first = jnp.minimum(before[:, ::TOKEN_BLOCK], capacity)
        last = jnp.concatenate([first[:, 1:], count[:, None]], axis=1)
        start = first // PIECE * PIECE
        length = jnp.where(last > first, last - start, 0)

        pack_pieces = (length[:experts] + PACK_ROWS - 1) // PACK_ROWS
        third, half = capacity // 4, capacity // 2
        order = [(0, 0, (capacity,)), (1, 0, (capacity,)), (1, 1, (capacity,)), (0, 1, (half,)),
                 (2, 0, (third, third, half)), (2, 1, (half, half)), (3, 0, (half, half)), (3, 1, (half, half)), (0, 1, (half,))]
        packed, results = {}, {}
        y = normed
        for r, i, sizes in order:
            own = slice(r * local, (r + 1) * local)
            if r not in packed:
                packed[r] = pack_rows(rows_of[r], slot[own], start[own].T.reshape(-1), pack_pieces[own].T.reshape(-1), capacity)
            done = results.setdefault((r, i), [])
            for size in sizes:
                y = expert_mlp(count[own], packed[r], w_gate, w_up, w_down, y, i, sum(part.shape[0] for part in done), size)
                done.append(exchange(y, r) if r else y)

        gates = sparse_gates(normed, w_router, choice, mask_first, mask_second)
        start, length, before, slot = start[experts:], length[experts:], before[experts:], slot[experts:]
        pieces = (length + PIECE - 1) // PIECE
        offset = (jnp.cumsum(pieces, axis=0) - pieces) * PIECE - start
        line = before + jnp.broadcast_to(offset[:, :, None], (experts, blocks, TOKEN_BLOCK)).reshape(experts, tokens)
        line = jnp.where(slot >= 0, line, -1)
        rows = [jnp.sum(jnp.where(near[j] == ids[:, None], line, 0), axis=0) for j in range(2)]
        sources = [results[r, i] for r in range(group_size) for i in range(local)]
        early = sources[:-1] + [sources[-1][:-1]]
        ready = (last[-1] <= capacity - sources[-1][-1].shape[0]).astype(jnp.int32)
        split = jnp.minimum(jnp.sum(ready), blocks - 1).reshape(1)
        operands = (hidden, jnp.stack(rows, axis=1), jnp.stack(gates, axis=1), split, start.T.reshape(-1), pieces.T.reshape(-1))
        out = combine(*operands, early)
        return combine(*operands, sources, out)

    return jax.shard_map(device_step, mesh=mesh,
                         in_specs=(rows_spec, P(), P(), P(), P("ep"), P("ep"), P("ep"), rows_spec, rows_spec, rows_spec),
                         out_specs=rows_spec, check_vma=False)
```

```python
import functools

import jax
import jax.numpy as jnp
from jax import lax
from jax.experimental import pallas as pl
from jax.experimental.pallas import tpu as pltpu
from jax.sharding import PartitionSpec as P


LN_EPS = 1e-5
TOKEN_BLOCK = 256
PIECE = 16
WIDE_PIECE = 64
PACK_BLOCK = 512
PACK_ROWS = 160
MLP_ROWS = 320


def norm_kernel(x_ref, gamma_ref, beta_ref, out_ref):
    values = x_ref[...].astype(jnp.float32)
    centred = values - jnp.mean(values, axis=-1, keepdims=True)
    variance = jnp.mean(centred * centred, axis=-1, keepdims=True)
    out_ref[...] = (centred * lax.rsqrt(variance + LN_EPS) * gamma_ref[...] + beta_ref[...]).astype(jnp.bfloat16)


def layer_norm(x, gamma, beta, block=512):
    tokens, d = x.shape
    row = pl.BlockSpec((1, d), lambda i: (0, 0))
    tile = pl.BlockSpec((block, d), lambda i: (i, 0))
    return pl.pallas_call(
        norm_kernel,
        grid=(tokens // block,),
        out_shape=jax.ShapeDtypeStruct((tokens, d), jnp.bfloat16),
        in_specs=[tile, row, row],
        out_specs=tile,
        compiler_params=pltpu.CompilerParams(vmem_limit_bytes=48 * 1024 * 1024),
        cost_estimate=pl.CostEstimate(flops=10 * tokens * d, bytes_accessed=4 * tokens * d, transcendentals=0),
        name="layer_norm",
    )(x, gamma.reshape(1, d), beta.reshape(1, d))


def sparse_gates(normed, w_router, choice, mask_first, mask_second):
    scores = jnp.dot(normed, w_router, preferred_element_type=jnp.float32)
    expert_ids = jnp.arange(w_router.shape[1], dtype=jnp.int32)

    def gate(mask, pick):
        soft_probs = jax.nn.softmax(jnp.where(mask > 0, scores, -jnp.inf), axis=-1)
        return jnp.sum(jnp.where(pick[:, None] == expert_ids, soft_probs, 0.0), axis=-1)

    return gate(mask_first, choice[:, 0]), gate(mask_second, choice[:, 1])


def pack_kernel(start_ref, pieces_ref, slot_ref, rows_ref, out_ref):
    block = pl.program_id(0)
    local, depth = out_ref.shape[0], out_ref.shape[1]
    tokens = rows_ref.shape[0]

    @pl.when(block == 0)
    def _():
        out_ref[...] = jnp.zeros_like(out_ref)

    pieces = pieces_ref[block * local]
    for i in range(1, local):
        pieces = jnp.maximum(pieces, pieces_ref[block * local + i])
    line = lax.broadcasted_iota(jnp.int32, (PACK_ROWS, tokens), 0)

    def one(p, _):
        at, picks = [], []
        for i in range(local):
            first = jnp.minimum(start_ref[block * local + i] + p * PACK_ROWS, depth - PACK_ROWS)
            at.append(pl.ds(pl.multiple_of(first, PIECE), PACK_ROWS))
            picks.append(jnp.where(slot_ref[i:i + 1, :] - first == line, 1.0, 0.0).astype(jnp.bfloat16))
        pick = jnp.concatenate(picks, axis=0)
        width = 256
        for c in range(0, rows_ref.shape[1], width):
            cols = slice(c, c + width)
            packed = jnp.dot(pick, rows_ref[:, cols], preferred_element_type=jnp.float32)
            for i in range(local):
                part = packed[i * PACK_ROWS:(i + 1) * PACK_ROWS]
                out_ref[i, at[i], cols] = (out_ref[i, at[i], cols].astype(jnp.float32) + part).astype(jnp.bfloat16)
        return 0

    lax.fori_loop(0, pieces, one, 0)


def pack_rows(rows, slot, start, pieces, capacity):
    tokens, d = rows.shape
    local = slot.shape[0]
    depth = capacity + PACK_ROWS
    return pl.pallas_call(
        pack_kernel,
        grid_spec=pltpu.PrefetchScalarGridSpec(
            num_scalar_prefetch=2,
            grid=(tokens // PACK_BLOCK,),
            in_specs=[pl.BlockSpec((local, PACK_BLOCK), lambda b, *_: (0, b)), pl.BlockSpec((PACK_BLOCK, d), lambda b, *_: (b, 0))],
            out_specs=pl.BlockSpec((local, depth, d), lambda b, *_: (0, 0, 0)),
        ),
        out_shape=jax.ShapeDtypeStruct((local, depth, d), jnp.bfloat16),
        compiler_params=pltpu.CompilerParams(vmem_limit_bytes=48 * 1024 * 1024),
        cost_estimate=pl.CostEstimate(flops=4 * tokens * d * PACK_ROWS, bytes_accessed=4 * tokens * d, transcendentals=0),
        name="pack_rows",
    )(start, pieces, slot, rows)


def mlp_kernel(e, origin, mb, ft, nt, cnt_ref, x_hbm, wg, wu, wd, prior, out_hbm, xv, wbuf, h, ov, xsem, wsem, osem):
    rows, d = out_hbm.shape
    f = wg.shape[2]
    fsteps, nsteps, sub = f // ft, d // nt, ft // 128
    panels = -(-f // d)
    nblk = lax.div(jnp.clip(cnt_ref[e] - origin, 0, rows) + (mb - 1), mb)

    def gu_copies(i, slot):
        out = []
        for j in range(sub):
            col = pl.ds(pl.multiple_of(i * ft + j * 128, 128), 128)
            out.append(pltpu.make_async_copy(wg.at[e, :, col], wbuf.at[slot, :, pl.ds(2 * j * 128, 128)], wsem.at[slot]))
            out.append(pltpu.make_async_copy(wu.at[e, :, col], wbuf.at[slot, :, pl.ds((2 * j + 1) * 128, 128)], wsem.at[slot]))
        return out

    def wd_copies(i, slot):
        out = []
        for k in range(panels):
            lines = min(d, f - k * d)
            col = pl.ds(pl.multiple_of(i * nt, nt), nt)
            out.append(pltpu.make_async_copy(wd.at[e, pl.ds(k * d, lines), col], wbuf.at[slot, pl.ds(0, lines), pl.ds(k * nt, nt)], wsem.at[slot]))
        return out

    def x_copy(m):
        at = pl.multiple_of(m * mb, mb)
        return pltpu.make_async_copy(x_hbm.at[e, pl.ds(at + origin, mb)], xv.at[pl.ds(at, mb)], xsem)

    def out_copy(i, slot):
        return pltpu.make_async_copy(ov.at[slot], out_hbm.at[:, pl.ds(pl.multiple_of(i * nt, nt), nt)], osem.at[slot])

    def each(copies, act):
        for c in copies:
            act(c)

    def loop(lo, hi, body):
        def step(m, _):
            body(m)
            return 0
        lax.fori_loop(lo, hi, step, 0)

    each(gu_copies(0, 0), lambda c: c.start())
    loop(0, nblk, lambda m: x_copy(m).start())
    loop(0, nblk, lambda m: x_copy(m).wait())

    def fstep(i):
        slot = lax.rem(i, 2)

        @pl.when(i + 1 < fsteps)
        def _():
            each(gu_copies(i + 1, 1 - slot), lambda c: c.start())

        @pl.when(i + 1 == fsteps)
        def _():
            each(wd_copies(0, fsteps % 2), lambda c: c.start())

        each(gu_copies(i, slot), lambda c: c.wait())

        def mstep(m):
            r = pl.ds(pl.multiple_of(m * mb, mb), mb)
            xb = xv[r, :]
            for j in range(sub):
                gu = jnp.dot(xb, wbuf[slot, :, pl.ds(2 * j * 128, 256)], preferred_element_type=jnp.float32)
                g, u = gu[:, :128], gu[:, 128:]
                h[i * sub + j, r, :] = (g * (1.0 / (1.0 + jnp.exp(-g))) * u).astype(jnp.bfloat16)

        loop(0, nblk, mstep)

    loop(0, fsteps, fstep)

    def nstep(i):
        slot, oslot = lax.rem(i + fsteps, 2), lax.rem(i, 2)

        @pl.when(i + 1 < nsteps)
        def _():
            each(wd_copies(i + 1, 1 - slot), lambda c: c.start())

        each(wd_copies(i, slot), lambda c: c.wait())

        @pl.when(i >= 2)
        def _():
            out_copy(i - 2, oslot).wait()

        def mstep(m):
            r = pl.ds(pl.multiple_of(m * mb, mb), mb)
            width = 256
            parts = []
            for k in range(panels):
                lines = min(d, f - k * d)
                parts.append(jnp.concatenate([h[q, r, :] for q in range(k * d // 128, (k * d + lines) // 128)], axis=1))
            for c in range(0, nt, width):
                acc = 0.0
                for k in range(panels):
                    lines = min(d, f - k * d)
                    acc += jnp.dot(parts[k], wbuf[slot, pl.ds(0, lines), pl.ds(k * nt + c, width)], preferred_element_type=jnp.float32)
                ov[oslot, r, pl.ds(c, width)] = acc.astype(jnp.bfloat16)

        loop(0, nblk, mstep)

        def zstep(m):
            ov[oslot, pl.ds(pl.multiple_of(m * mb, mb), mb), :] = jnp.zeros((mb, nt), jnp.bfloat16)

        loop(nblk, rows // mb, zstep)
        out_copy(i, oslot).start()

    loop(0, nsteps, nstep)
    for i in range(max(nsteps - 2, 0), nsteps):
        out_copy(i, i % 2).wait()


def expert_mlp(cnt, x, wg, wu, wd, prior, e, origin, rows, mb=MLP_ROWS):
    d, f = wg.shape[1:]
    ft = 1152 if f % 1152 == 0 else 640
    nt = 768 if d % 768 == 0 else 256
    any_ = pl.BlockSpec(memory_space=pl.ANY)
    return pl.pallas_call(
        functools.partial(mlp_kernel, e, origin, mb, ft, nt),
        out_shape=jax.ShapeDtypeStruct((rows, d), jnp.bfloat16),
        in_specs=[pl.BlockSpec(memory_space=pltpu.SMEM)] + [any_] * 5,
        out_specs=any_,
        scratch_shapes=[pltpu.VMEM((rows, d), jnp.bfloat16), pltpu.VMEM((2, d, 2 * ft), jnp.bfloat16),
                        pltpu.VMEM((f // 128, rows, 128), jnp.bfloat16), pltpu.VMEM((2, rows, nt), jnp.bfloat16),
                        pltpu.SemaphoreType.DMA, pltpu.SemaphoreType.DMA((2,)), pltpu.SemaphoreType.DMA((2,))],
        compiler_params=pltpu.CompilerParams(vmem_limit_bytes=60 * 1024 * 1024),
        cost_estimate=pl.CostEstimate(flops=6 * rows * d * f, bytes_accessed=6 * d * f + 4 * rows * d, transcendentals=0),
        name="expert_mlp",
    )(cnt, x, wg, wu, wd, prior)


def combine_kernel(parts, tail, split_ref, start_ref, pieces_ref, x_ref, row_ref, gate_ref, *refs):
    refs, out_ref, rows_buf, sem = list(refs[:-3]), refs[-3], refs[-2], refs[-1]
    sources = [[refs.pop(0) for _ in range(n)] for n in parts]
    step, steps = pl.program_id(0), pl.num_programs(0)
    lo, hi = (split_ref[0], steps) if tail else (0, split_ref[0])
    experts = len(sources)
    depth = rows_buf.shape[1]

    def each_piece(block, act):
        slot = lax.rem(block, 2)
        base = jnp.int32(0)
        for e, source in enumerate(sources):
            start, pieces = start_ref[block * experts + e], pieces_ref[block * experts + e]
            end, offset = start + pieces * PIECE, 0
            for part in source:
                size = part.shape[0]
                low, high = jnp.clip(start - offset, 0, size), jnp.clip(end - offset, 0, size)
                offset += size
                wide = lax.div(high - low, WIDE_PIECE)

                def one(rows, p, at, part=part, low=low):
                    src = part.at[pl.ds(pl.multiple_of(low + (at - p), PIECE), rows)]
                    dst = rows_buf.at[slot, pl.ds(pl.multiple_of(at, PIECE), rows)]
                    act(pltpu.make_async_copy(src, dst, sem.at[slot]))
                    return at + rows

                first = base
                base = lax.fori_loop(0, wide, lambda p, at: one(WIDE_PIECE, first, at), base)
                base = lax.fori_loop(0, lax.div(high - low - wide * WIDE_PIECE, PIECE), lambda p, at: one(PIECE, first, at), base)

    @pl.when(step == 0)
    def _():
        rows_buf[...] = jnp.zeros_like(rows_buf)

    @pl.when((step == lo) & (step < hi))
    def _():
        each_piece(step, lambda c: c.start())

    @pl.when((step >= lo) & (step + 1 < hi))
    def _():
        each_piece(step + 1, lambda c: c.start())

    @pl.when((step >= lo) & (step < hi))
    def _():
        each_piece(step, lambda c: c.wait())
        slot = lax.rem(step, 2)
        lane = lax.broadcasted_iota(jnp.int32, (x_ref.shape[0], depth), 1)
        first = jnp.where(lane == row_ref[:, 0:1], 1.0, 0.0).astype(jnp.bfloat16)
        second = jnp.where(lane == row_ref[:, 1:2], 1.0, 0.0).astype(jnp.bfloat16)
        width = 256
        for c in range(0, x_ref.shape[1], width):
            cols = slice(c, c + width)
            rows = rows_buf[slot, :, cols]
            y_first = jnp.dot(first, rows, preferred_element_type=jnp.float32)
            y_second = jnp.dot(second, rows, preferred_element_type=jnp.float32)
            mixed = gate_ref[:, 0:1] * y_first + gate_ref[:, 1:2] * y_second
            out_ref[:, cols] = (x_ref[:, cols].astype(jnp.float32) + mixed).astype(jnp.bfloat16)


def combine(x, rows, gates, split, start, pieces, sources, earlier=None):
    tokens, d = x.shape
    depth = -(-(2 * TOKEN_BLOCK + len(sources) * (2 * PIECE - 2)) // 256) * 256
    tail = earlier is not None
    block = (lambda i, s, *_: (jnp.maximum(i, s[0]), 0)) if tail else (lambda i, s, *_: (jnp.clip(i, 0, jnp.maximum(s[0] - 1, 0)), 0))
    tile = pl.BlockSpec((TOKEN_BLOCK, d), block)
    pair = pl.BlockSpec((TOKEN_BLOCK, 2), block)
    flat = sum(sources, []) + ([earlier] if tail else [])
    return pl.pallas_call(
        functools.partial(combine_kernel, [len(s) for s in sources], tail),
        grid_spec=pltpu.PrefetchScalarGridSpec(
            num_scalar_prefetch=3,
            grid=(tokens // TOKEN_BLOCK,),
            in_specs=[tile, pair, pair] + [pl.BlockSpec(memory_space=pl.ANY)] * len(flat),
            out_specs=tile,
            scratch_shapes=[pltpu.VMEM((2, depth, d), jnp.bfloat16), pltpu.SemaphoreType.DMA((2,))],
        ),
        out_shape=jax.ShapeDtypeStruct((tokens, d), jnp.bfloat16),
        input_output_aliases={len(flat) + 5: 0} if tail else {},
        compiler_params=pltpu.CompilerParams(vmem_limit_bytes=40 * 1024 * 1024),
        cost_estimate=pl.CostEstimate(flops=4 * tokens * depth * d, bytes_accessed=16 * tokens * d, transcendentals=0),
        name="combine",
    )(split, start, pieces, x, rows, gates, *flat)


def solution(mesh):
    group_size = mesh.shape["ep"]
    rows_spec = P(("dp", "ep"))

    def exchange(value, distance):
        return lax.ppermute(value, "ep", [(k, k ^ distance) for k in range(group_size)])

    def device_step(hidden, ln_gamma, ln_beta, w_router, w_gate, w_up, w_down, choice, mask_first, mask_second):
        tokens, d = hidden.shape
        local = w_gate.shape[0]
        experts = local * group_size
        capacity = (10 * tokens + 4 * experts - 1) // (4 * experts)
        blocks = tokens // TOKEN_BLOCK
        choices = [choice.T] + [exchange(choice.T, r) for r in range(1, group_size)]
        ln_gamma, choices = lax.optimization_barrier((ln_gamma, choices))
        normed = layer_norm(hidden, ln_gamma, ln_beta)
        rows_of = {0: normed, 1: exchange(normed, 1), 2: exchange(normed, 2)}
        rows_of[3] = exchange(rows_of[2], 1)

        me = lax.axis_index("ep")
        here = me * local + jnp.arange(local, dtype=jnp.int32)
        near = choice.T ^ (me * local)
        ids = jnp.arange(experts, dtype=jnp.int32)
        hit = [jnp.any(c[:, None, :] == here[:, None], axis=0) for c in choices] + [jnp.any(near[:, None, :] == ids[:, None], axis=0)]
        hit = jnp.concatenate(hit, axis=0).astype(jnp.int32)
        after = jnp.cumsum(hit, axis=1)
        before = after - hit
        count = jnp.minimum(after[:, -1], capacity)
        slot = jnp.where((hit > 0) & (before < capacity), before, -1)
        first = jnp.minimum(before[:, ::TOKEN_BLOCK], capacity)
        last = jnp.concatenate([first[:, 1:], count[:, None]], axis=1)
        start = first // PIECE * PIECE
        length = jnp.where(last > first, last - start, 0)

        step = PACK_BLOCK // TOKEN_BLOCK
        pack_start = start[:experts, ::step]
        pack_pieces = jnp.maximum(last[:experts, step - 1::step] - pack_start + PACK_ROWS - 1, 0) // PACK_ROWS
        half, whole = (capacity // 2,), (capacity,)
        order = [(0, 0, whole), (1, 0, whole), (1, 1, whole), (0, 1, half), (2, 0, half + half), (2, 1, whole),
                 (3, 0, whole), (3, 1, half + half), (0, 1, half)]
        packed, results = {}, {}
        y = normed
        for r, i, sizes in order:
            own = slice(r * local, (r + 1) * local)
            if r not in packed:
                packed[r] = pack_rows(rows_of[r], slot[own], pack_start[own].T.reshape(-1), pack_pieces[own].T.reshape(-1), capacity)
            done = results.setdefault((r, i), [])
            for size in sizes:
                y = expert_mlp(count[own], packed[r], w_gate, w_up, w_down, y, i, sum(part.shape[0] for part in done), size)
                done.append(exchange(y, r) if r else y)

        gates = sparse_gates(normed, w_router, choice, mask_first, mask_second)
        start, length, before, slot = start[experts:], length[experts:], before[experts:], slot[experts:]
        pieces = (length + PIECE - 1) // PIECE
        offset = (jnp.cumsum(pieces, axis=0) - pieces) * PIECE - start
        line = before + jnp.broadcast_to(offset[:, :, None], (experts, blocks, TOKEN_BLOCK)).reshape(experts, tokens)
        line = jnp.where(slot >= 0, line, -1)
        rows = [jnp.sum(jnp.where(near[j] == ids[:, None], line, 0), axis=0) for j in range(2)]
        sources = [results[r, i] for r in range(group_size) for i in range(local)]
        early = sources[:-1] + [sources[-1][:-1]]
        ready = (last[-1] <= capacity - sources[-1][-1].shape[0]).astype(jnp.int32)
        split = jnp.minimum(jnp.sum(ready), blocks - 1).reshape(1)
        operands = (hidden, jnp.stack(rows, axis=1), jnp.stack(gates, axis=1), split, start.T.reshape(-1), pieces.T.reshape(-1))
        out = combine(*operands, early)
        return combine(*operands, sources, out)

    return jax.shard_map(device_step, mesh=mesh,
                         in_specs=(rows_spec, P(), P(), P(), P("ep"), P("ep"), P("ep"), rows_spec, rows_spec, rows_spec),
                         out_specs=rows_spec, check_vma=False)
```
